1024 devices in a mesh: gx: 16 (over z_hi, x, core), gy: 4 (over y), gz: 16 (over z_lo).
Axes of the slice: x: 4, y: 4, z: 32 (z_hi: 2, z_lo: 16; z = z_hi * 16 + z_lo), core: 2. Of those that a mesh axis runs over, the one named last changes fastest.
Arguments:
- solution: float32 [16, 32, 64, 512], P(None, 'gx', 'gz', 'gy'), may hold values from -0.6 to 0.6
- residual: float32 [16, 32, 64, 512], P(None, 'gx', 'gz', 'gy'), may hold values from -6 to 6
- direction_prev: float32 [16, 32, 64, 512], P(None, 'gx', 'gz', 'gy'), may hold values from -0.3 to 0.3, as said below
- image_prev: float32 [16, 32, 64, 512], P(None, 'gx', 'gz', 'gy'), may hold values from -9 to 9, as said below
- gram_prev: float32 [16, 16], replicated, may hold values from -1048576 to 1048576, as said below
Outputs:
- solution_new: float32 [16, 32, 64, 512], P(None, 'gx', 'gz', 'gy')
- residual_new: float32 [16, 32, 64, 512], P(None, 'gx', 'gz', 'gy')
- direction: float32 [16, 32, 64, 512], P(None, 'gx', 'gz', 'gy')
The draws below stay inside these ranges and needn't reach their ends.
Inputs may be any that keep to these rules, and one draw needn't show every extreme that they name: direction_prev is a field of order 0.05. image_prev equals A direction_prev, computed in float32. gram_prev is symmetric and positive definite.
All inputs are finite; a program needn't handle non-finite values.
Results may differ from the reference program's by a relative error of at most 0.0001.
Values sent between devices are 32-bit elements; how exact they have to be, the bound alone decides.
A program may use at most 64 MiB of HBM per device.

```python
import jax
import jax.numpy as jnp
from jax import lax

RHS = 16
NX = 32
NZ = 64
NY = 512


def box_total(padded):
    total = padded[:, :-2] + padded[:, 1:-1] + padded[:, 2:]
    total = total[:, :, :-2] + total[:, :, 1:-1] + total[:, :, 2:]
    return total[:, :, :, :-2] + total[:, :, :, 1:-1] + total[:, :, :, 2:]


def shared_fields(key):
    base = jax.random.fold_in(key, 11)
    shape = (RHS, NX, NZ, NY)
    field = jnp.clip(0.04 * jax.random.normal(base, shape, jnp.float32), -0.24, 0.24)
    padded = jnp.pad(field, ((0, 0), (1, 1), (1, 1), (1, 1)))
    image = 27.0 * field - box_total(padded)
    return (field, image)


def draw_direction_prev(key, part):
    return shared_fields(key)[0]


def draw_image_prev(key, part):
    return shared_fields(key)[1]


def draw_gram_prev(key, part):
    base = jax.random.fold_in(key, 23)
    noise = jax.random.normal(base, (RHS, RHS), jnp.float32)
    matrix = jnp.eye(RHS, dtype=jnp.float32) + 0.05 * (noise + noise.T)
    return matrix * (NX * NY * NZ / 20.0)


def block_scale(key, extent, cuts, smallest, high):
    factor_of, own = 1.0, jax.random.fold_in(key, 6)
    for dim, parts in cuts:
        steps = jnp.exp(jax.random.uniform(jax.random.fold_in(own, dim), (parts,), jnp.float32, smallest / len(cuts), high / len(cuts)))
        factor_of = factor_of * jnp.repeat(steps, extent[dim] // parts).reshape([-1 if axis == dim else 1 for axis in range(len(extent))])
    return factor_of


def gaussian(key, extent, scale, limit, shards=(), kind=jnp.bfloat16):
    level = block_scale(key, extent, shards, -0.22, 0.18) if shards else 1.0
    drawn = jax.random.normal(key, extent, jnp.float32) * scale * level
    return jnp.minimum(jnp.maximum(drawn, -limit), limit).astype(kind)


def setup_inputs(seed: int = 0) -> dict:
    key_of = jax.random.split(jax.random.key(seed), 6)
    return {
        "solution": gaussian(key_of[0], (RHS, NX, NZ, NY), 0.1, 0.6, ((1, 16), (2, 16), (3, 4)), jnp.float32),
        "residual": gaussian(key_of[1], (RHS, NX, NZ, NY), 1.0, 6.0, ((1, 16), (2, 16), (3, 4)), jnp.float32),
        "direction_prev": draw_direction_prev(jax.random.fold_in(key_of[5], 71), 0),
        "image_prev": draw_image_prev(jax.random.fold_in(key_of[5], 71), 0),
        "gram_prev": draw_gram_prev(jax.random.fold_in(key_of[5], 71), 0),
    }


def pad_field(field):
    return jnp.pad(field, ((0, 0), (1, 1), (1, 1), (1, 1)))

def box_sum(padded):
    total = padded[:, :-2] + padded[:, 1:-1] + padded[:, 2:]
    total = total[:, :, :-2] + total[:, :, 1:-1] + total[:, :, 2:]
    return total[:, :, :, :-2] + total[:, :, :, 1:-1] + total[:, :, :, 2:]

def colors_of(shape):
    first = lax.broadcasted_iota(jnp.int32, shape, 1) % 2
    second = lax.broadcasted_iota(jnp.int32, shape, 2) % 2
    third = lax.broadcasted_iota(jnp.int32, shape, 3) % 2
    return 4 * first + 2 * second + third

def gram(left, right):
    return jnp.einsum('kxzy,lxzy->kl', left, right, precision=lax.Precision.HIGHEST)

def combine(field, mixing):
    return jnp.einsum('kxzy,kl->lxzy', field, mixing, precision=lax.Precision.HIGHEST)

def spd_solve(matrix, target):
    order = matrix.shape[0]
    sym = 0.5 * (matrix + matrix.T)
    lower = jnp.zeros_like(sym)
    for col in range(order):
        column = sym[col:, col] - lax.optimization_barrier(jnp.sum(lower[col:, :col] * lower[col, :col][None, :], axis=1))
        pivot = jnp.sqrt(column[0])
        lower = lower.at[col:, col].set(column / pivot)
    middle = jnp.zeros_like(target)
    for row in range(order):
        value = target[row] - lax.optimization_barrier(jnp.sum(lower[row, :row][:, None] * middle[:row], axis=0))
        middle = middle.at[row].set(value / lower[row, row])
    answer = jnp.zeros_like(target)
    for row in range(order - 1, -1, -1):
        value = middle[row] - lax.optimization_barrier(jnp.sum(lower[row + 1:, row][:, None] * answer[row + 1:], axis=0))
        answer = answer.at[row].set(value / lower[row, row])
    return answer

def reference(solution, residual, direction_prev, image_prev, gram_prev):
    colors = colors_of(residual.shape)
    smoothed = jnp.where(colors == 0, residual / 26.0, jnp.float32(0.0))
    for shade in list(range(1, 8)) + list(range(6, -1, -1)):
        boxed = box_sum(pad_field(smoothed))
        smoothed = jnp.where(colors == shade, (residual + boxed - smoothed) / 26.0, smoothed)
    image = 27.0 * smoothed - box_sum(pad_field(smoothed))
    gram_zr = gram(smoothed, residual)
    beta_mix = spd_solve(gram_prev, gram_zr)
    direction = smoothed + combine(direction_prev, beta_mix)
    image_new = image + combine(image_prev, beta_mix)
    curvature = gram(direction, image_new)
    alpha_step = spd_solve(curvature, gram_zr)
    solution_new = solution + combine(direction, alpha_step)
    residual_new = residual - combine(image_new, alpha_step)
    return (solution_new, residual_new, direction)
```

```python
import functools

import jax
import jax.numpy as jnp
from jax import lax
from jax.experimental import pallas as pl
from jax.experimental.pallas import tpu as pltpu
from jax.sharding import PartitionSpec as P

RHS = 16
LX = 2
LZ = 4
LY = 128
LINES = LX * LZ
WIDE = 2 * LY
LO0, HI0 = 2, 1
LO1, HI1 = 4, 3
N0 = LO0 + LZ + HI0
N1 = LO1 + LZ + HI1
CORES = 2
HIGHEST = lax.Precision.HIGHEST
MESH = pl.DeviceIdType.MESH
AXES = ("gx", "gy", "gz")


class Place:
    def __init__(self, sizes, xs):
        self.gx, self.gy, self.gz = sizes
        self.xs = xs
        self.zs = self.gx // (CORES * xs) * self.gz
        self.g, self.m, self.h = (lax.axis_index(a) for a in AXES)
        self.core = lax.rem(self.g, CORES)
        self.x = lax.rem(self.g // CORES, xs)
        self.z = self.g // (CORES * xs) * self.gz + self.h

    def chip(self, dx, dy, dz, other_core=False):
        x = lax.rem(self.x + dx + self.xs, self.xs)
        y = lax.rem(self.m + dy + self.gy, self.gy)
        z = lax.rem(self.z + dz + self.zs, self.zs)
        core = 1 - self.core if other_core else self.core
        return (z // self.gz * (CORES * self.xs) + x * CORES + core, y, lax.rem(z, self.gz))


def plane_offsets(place):
    return [(dx, dy) for dx in range(place.xs) for dy in range(place.gy) if (dx, dy) != (0, 0)]


def window_of(zs):
    return 4 if zs > 4 else 2


def window_offsets(zs):
    return (-1, 1, 2) if window_of(zs) == 4 else (1,)


def stride_offsets(zs):
    return list(range(window_of(zs), zs, window_of(zs)))


def sides(value):
    return pltpu.roll(value, 1, 1) + pltpu.roll(value, WIDE - 1, 1)


def ybox(value):
    return value + sides(value)


def line_of(ref, line):
    return ref[pl.ds(line, RHS, stride=LINES), :]


def invert(matrix, target, order):
    rows = lax.broadcasted_iota(jnp.int32, (order, 128), 0)
    columns = [jnp.broadcast_to(matrix[:, j : j + 1], (order, 128)) for j in range(order)]
    for k in range(order):
        pivot = 1.0 / jnp.broadcast_to(columns[k][k : k + 1, :], (order, 128))
        own = rows == k
        for j in range(k + 1, order):
            scaled = jnp.broadcast_to(columns[j][k : k + 1, :], (order, 128)) * pivot
            columns[j] = jnp.where(own, scaled, columns[j] - columns[k] * scaled)
        scaled = jnp.broadcast_to(target[k : k + 1, :], (order, 128)) * pivot
        target = jnp.where(own, scaled, target - columns[k] * scaled)
    return target


def exchange_kernel(
    sizes, xs,
    res_ref, dirp_ref, imgp_ref, gram_ref,
    smooth_ref, image_ref, total_ref, inverse_ref,
    r0, r1, up, down, upin, downin, f_ref, s1, s0, masks, y_ref, send3, u3, u3in,
    ar_send, ar_in,
    send0, recv0, send1, recv1, send2, recv2, send3s, recv3s, send_ar, recv_ar,
):
    place = Place(sizes, xs)
    g, m, h = place.g, place.m, place.h
    zero = jnp.zeros((RHS, LY), jnp.float32)
    below_z, above_z = h > 0, h < place.gz - 1
    below_y, above_y = m > 0, m < place.gy - 1
    below_x, above_x = g > 0, g < place.gx - 1

    @pl.when(jnp.logical_not(below_z & above_z & below_y & above_y & below_x & above_x))
    def _():
        for i in range(N0):
            for s in range(3):
                r0[s, i] = zero
        for p in range(2):
            for i in range(N1):
                for s in range(3):
                    r1[p, s, i] = zero
        for j in range(LZ):
            upin[j] = zero
            downin[j] = zero
            u3in[j] = zero
        s0[LZ + 1] = jnp.zeros((RHS, WIDE), jnp.float32)

    barrier = pltpu.get_barrier_semaphore()
    near = []
    for dz in (-1, 0, 1):
        for dy in (-1, 0, 1):
            if (dz, dy) != (0, 0):
                cond = True
                cond = cond & (below_z if dz < 0 else above_z) if dz else cond
                cond = cond & (below_y if dy < 0 else above_y) if dy else cond
                near.append((cond, (g, m + dy, h + dz)))
    near.append((below_x, (g - 1, m, h)))
    near.append((above_x, (g + 1, m, h)))
    always = [place.chip(0, 0, 0, True)]
    always += [place.chip(dx, dy, 0) for dx, dy in plane_offsets(place)]
    offs = set(window_offsets(place.zs)) | {-o for o in window_offsets(place.zs)} | set(stride_offsets(place.zs))
    always += [place.chip(0, 0, dz) for dz in sorted({o % place.zs for o in offs})]
    expected = len(always)
    for cond, device in near:
        expected = expected + jnp.where(cond, 1, 0)

        @pl.when(cond)
        def _(device=device):
            pl.semaphore_signal(barrier, inc=1, device_id=device, device_id_type=MESH)

    for device in always:
        pl.semaphore_signal(barrier, inc=1, device_id=device, device_id_type=MESH)

    lane = lax.broadcasted_iota(jnp.int32, (RHS, WIDE), 1)
    inside = (lane < LY) | ((lane < LY + LY // 2) & above_y) | ((lane >= LY + LY // 2) & below_y)
    scale = jnp.where(inside, jnp.float32(1 / 26), jnp.float32(0))
    even = jnp.where(lax.rem(lane, 2) == 0, scale, jnp.float32(0))
    odd = scale - even
    for t, keep in enumerate((True, below_z, above_z)):
        weight = jnp.float32(1) if t == 0 else jnp.where(keep, jnp.float32(1), jnp.float32(0))
        masks[t, 0] = even * weight
        masks[t, 1] = odd * weight
    for j in range(LZ):
        r0[0, LO0 + j] = line_of(res_ref, j)
    ident = jnp.where(
        lax.broadcasted_iota(jnp.int32, (RHS, 128), 0) == lax.broadcasted_iota(jnp.int32, (RHS, 128), 1),
        jnp.float32(1), jnp.float32(0),
    )
    gram = gram_ref[...]
    sym = 0.5 * (gram + gram.T)
    inverse_ref[...] = invert(sym, ident, RHS)
    gram_pq = jnp.zeros((RHS, 128), jnp.float32)
    for line in range(LINES):
        right = jnp.concatenate([zero[:8]] * 6 + [line_of(imgp_ref, line)] + [zero[:8]] * 8, axis=0)
        gram_pq += lax.dot_general(
            line_of(dirp_ref, line), right, (((1,), (1,)), ((), ())), precision=HIGHEST, preferred_element_type=jnp.float32
        )

    pl.semaphore_wait(barrier, expected)

    def mask(j, parity):
        return masks[0 if 0 <= j < LZ else 1 if j < 0 else 2, parity]

    def start(copies):
        for cond, copy in copies:
            pl.when(cond)(copy.start)

    def finish(copies):
        for cond, copy in copies:
            pl.when(cond)(copy.wait_send)

    def around(buf, low, high, before, send_sems, recv_sems):
        out = []
        cond_z = {-1: below_z, 1: above_z}
        cond_y = {-1: below_y, 1: above_y}
        n = 0
        for dz in (0, 1, -1):
            for dy in (0, 1, -1):
                if (dz, dy) == (0, 0):
                    continue
                src, size = (low, LZ) if dz == 0 else (low + LZ - before, before) if dz > 0 else (low, high)
                dst = low if dz == 0 else 0 if dz > 0 else low + LZ
                slot = 0 if dy == 0 else 1 if dy > 0 else 2
                copy = pltpu.make_async_remote_copy(
                    src_ref=buf.at[0, pl.ds(src, size)],
                    dst_ref=buf.at[slot, pl.ds(dst, size)],
                    send_sem=send_sems.at[n], recv_sem=recv_sems.at[n],
                    device_id=(g, m + dy, h + dz), device_id_type=MESH,
                )
                to, came = True, True
                if dz:
                    to, came = to & cond_z[dz], came & cond_z[-dz]
                if dy:
                    to, came = to & cond_y[dy], came & cond_y[-dy]
                out.append((to, came, copy))
                n += 1
        return out

    def wide(buf, i):
        lane_half = lax.broadcasted_iota(jnp.int32, (RHS, LY), 1) < LY // 2
        return jnp.concatenate([buf[0, i], jnp.where(lane_half, buf[2, i], buf[1, i])], axis=1)

    copies0 = around(r0, LO0, HI0, LO0, send0, recv0)
    start([(to, copy) for to, _, copy in copies0])
    for _, came, copy in copies0:
        pl.when(came)(copy.wait_recv)

    rw = {j: wide(r0, LO0 + j) for j in range(-LO0, LZ + HI0)}
    fe = {}
    for j in range(-LO0, LZ + HI0, 2):
        e = rw[j] * mask(j, 0)
        o = (rw[j] + sides(e)) * mask(j, 1)
        fe[j] = e
        f_ref[LO0 + j] = e + o
    for j in range(-1, LZ, 2):
        n = rw[j] + ybox(f_ref[LO0 + j - 1] + f_ref[LO0 + j + 1])
        e = n * mask(j, 0)
        o = (n + sides(e)) * mask(j, 1)
        fe[j] = e
        f_ref[LO0 + j] = e + o

    for j in range(LZ):
        box = ybox(f_ref[LO0 + j - 1] + f_ref[LO0 + j] + f_ref[LO0 + j + 1])[:, :LY]
        down[j] = box
        up[j] = line_of(res_ref, LZ + j) + box
    to_up = pltpu.make_async_remote_copy(
        src_ref=up, dst_ref=upin, send_sem=send1.at[0], recv_sem=recv1.at[0], device_id=(g + 1, m, h), device_id_type=MESH
    )
    to_down = pltpu.make_async_remote_copy(
        src_ref=down, dst_ref=downin, send_sem=send1.at[1], recv_sem=recv1.at[1], device_id=(g - 1, m, h), device_id_type=MESH
    )
    start([(above_x, to_up), (below_x, to_down)])

    pl.when(below_x)(to_up.wait_recv)
    keep = jnp.where(below_x, jnp.float32(1), jnp.float32(0))
    for j in range(LZ):
        r1[0, 0, LO1 + j] = (upin[j] + down[j]) * keep
    low = around(r1.at[0], LO1, HI1, LO1, send2.at[0], recv2.at[0])
    start([(to, copy) for to, _, copy in low])
    pl.when(above_x)(to_down.wait_recv)
    for j in range(LZ):
        r1[1, 0, LO1 + j] = downin[j] + up[j]
    high = around(r1.at[1], LO1, HI1, LO1, send2.at[1], recv2.at[1])
    start([(to, copy) for to, _, copy in high])
    for _, came, copy in low + high:
        pl.when(came)(copy.wait_recv)

    for p in range(2):
        r = {j: wide(r1.at[p], LO1 + j) for j in range(-LO1, LZ + HI1)}
        evens = {}
        for j in range(-LO1, LZ + HI1, 2):
            e = r[j] * mask(j, 0)
            o = (r[j] + sides(e)) * mask(j, 1)
            evens[j] = e
            s1[p, LO1 + j] = e + o
        for j in range(1 - LO1, LZ + HI1 - 1, 2):
            n = r[j] + ybox(s1[p, LO1 + j - 1] + s1[p, LO1 + j + 1])
            e = n * mask(j, 0)
            o = (n + sides(e)) * mask(j, 1)
            e = (n + sides(o)) * mask(j, 0)
            s1[p, LO1 + j] = e + o
        for j in range(2 - LO1, LZ + HI1 - 2, 2):
            n = r[j] + ybox(s1[p, LO1 + j - 1] + s1[p, LO1 + j + 1])
            o = (n + sides(evens[j])) * mask(j, 1)
            e = (n + sides(o)) * mask(j, 0)
            s1[p, LO1 + j] = e + o

    def odd_sum(j):
        both = [s1[0, LO1 + i] + s1[1, LO1 + i] for i in (j - 1, j, j + 1)]
        return ybox(both[0] + both[1] + both[2])

    for j in range(-1, LZ):
        y_ref[1 + j] = odd_sum(j)
    for j in range(-1, LZ, 2):
        n = rw[j] + y_ref[1 + j] + ybox(f_ref[LO0 + j - 1] + f_ref[LO0 + j + 1])
        o = (n + sides(fe[j])) * mask(j, 1)
        e = (n + sides(o)) * mask(j, 0)
        s0[1 + j] = e + o
    for j in range(0, LZ, 2):
        n = rw[j] + y_ref[1 + j] + ybox(s0[1 + j - 1] + s0[1 + j + 1])
        o = (n + sides(fe[j])) * mask(j, 1)
        e = (n + sides(o)) * mask(j, 0)
        s0[1 + j] = e + o

    send3[...] = s0[1]
    to_z = pltpu.make_async_remote_copy(
        src_ref=send3, dst_ref=s0.at[LZ + 1], send_sem=send3s.at[0], recv_sem=recv3s.at[0],
        device_id=(g, m, h - 1), device_id_type=MESH,
    )
    start([(below_z, to_z)])

    sums = gram_pq
    for a in range(LX):
        for j in range(LZ):
            line = a * LZ + j
            own = s0[1 + j] if a == 0 else s1[1, LO1 + j]
            if a == 0:
                half = y_ref[1 + j] + ybox(s0[j]) + pltpu.roll(own, 1, 1)
            else:
                half = ybox(s1[1, LO1 + j - 1]) + pltpu.roll(own, 1, 1)
            half = (13.0 * own - half)[:, :LY]
            own = own[:, :LY]
            smooth_ref[line] = own
            right = jnp.concatenate([line_of(res_ref, line), line_of(imgp_ref, line), half] + [zero[:8]] * 10, axis=0)
            sums += lax.dot_general(
                own, right, (((1,), (1,)), ((), ())), precision=HIGHEST, preferred_element_type=jnp.float32
            )
    value = sums[:8] + pltpu.roll(sums[8:], 64, 1)

    def to_all(devices, value, slot):
        ar_send[slot] = value
        copies = []
        for i, device in enumerate(devices):
            copies.append(
                pltpu.make_async_remote_copy(
                    src_ref=ar_send.at[slot], dst_ref=ar_in.at[first[slot] + i],
                    send_sem=send_ar.at[first[slot] + i], recv_sem=recv_ar.at[first[slot] + i],
                    device_id=device, device_id_type=MESH,
                )
            )
        for copy in copies:
            copy.start()
        return copies

    def collect(copies, value, slot):
        for i, copy in enumerate(copies):
            copy.wait_recv()
            value = value + ar_in[first[slot] + i]
        return value

    groups = [
        [place.chip(0, 0, 0, True)],
        [place.chip(dx, dy, 0) for dx, dy in plane_offsets(place)],
        [place.chip(0, 0, -dz) for dz in window_offsets(place.zs)],
        [place.chip(0, 0, dz) for dz in stride_offsets(place.zs)],
    ]
    first = [sum(len(q) for q in groups[:i]) for i in range(len(groups))]
    sent = []
    for slot in range(3):
        copies = to_all(groups[slot], value, slot)
        sent += copies
        value = collect(copies, value, slot)
        if slot == 0:
            pl.when(above_z)(to_z.wait_recv)
            for j in range(LZ):
                u3[j] = ybox(s0[j] + s0[1 + j] + s0[2 + j])[:, :LY]
            to_x = pltpu.make_async_remote_copy(
                src_ref=u3, dst_ref=u3in, send_sem=send3s.at[1], recv_sem=recv3s.at[1],
                device_id=(g - 1, m, h), device_id_type=MESH,
            )
            start([(below_x, to_x)])
    copies = to_all(groups[3], value, 3)
    sent += copies
    for j in range(LZ):
        image_ref[j] = 27.0 * s0[1 + j][:, :LY] - (y_ref[1 + j][:, :LY] + u3[j])
    pl.when(above_x)(to_x.wait_recv)
    for j in range(LZ):
        box = ybox(s1[1, LO1 + j - 1] + s1[1, LO1 + j] + s1[1, LO1 + j + 1])[:, :LY]
        image_ref[LZ + j] = 27.0 * s1[1, LO1 + j][:, :LY] - (box + u3[j] + u3in[j])
    value = collect(copies, value, 3)
    total_ref[...] = value

    finish([(to, copy) for to, _, copy in copies0 + low + high])
    finish([(above_x, to_up), (below_x, to_down), (below_z, to_z), (below_x, to_x)])
    for copy in sent:
        copy.wait_send()


def update_kernel(
    sol_ref, res_ref, dirp_ref, imgp_ref, smooth_ref, image_ref, total_ref, inverse_ref, sol_out, res_out, dir_out
):
    def dot(a, b, ca=1, cb=0):
        return lax.dot_general(a, b, (((ca,), (cb,)), ((), ())), precision=HIGHEST, preferred_element_type=jnp.float32)

    total = total_ref[...]
    both = jnp.concatenate([total, pltpu.roll(total, 64, 1)], axis=0)
    gram, cross, half, prev = (both[:, RHS * i : RHS * (i + 1)] for i in range(4))
    beta = dot(inverse_ref[...][:, :RHS], gram)
    mixed = dot(cross, beta)
    curved = half + mixed
    curvature = curved + curved.T + dot(beta, dot(0.5 * (prev + prev.T), beta), 0, 0)
    curvature = 0.5 * (curvature + curvature.T)
    alpha = invert(curvature, jnp.concatenate([gram] * 8, axis=1), RHS)[:, :RHS]

    def all_lines(ref):
        return jnp.concatenate([line_of(ref, line) for line in range(LINES)], axis=1)

    smooth = jnp.concatenate([smooth_ref[line] for line in range(LINES)], axis=1)
    image = jnp.concatenate([image_ref[line] for line in range(LINES)], axis=1)
    direction = smooth + dot(beta, all_lines(dirp_ref), 0, 0)
    image_new = image + dot(beta, all_lines(imgp_ref), 0, 0)
    sol_new = all_lines(sol_ref) + dot(alpha, direction, 0, 0)
    res_new = all_lines(res_ref) - dot(alpha, image_new, 0, 0)
    for line in range(LINES):
        at = slice(line * LY, (line + 1) * LY)
        dir_out[pl.ds(line, RHS, stride=LINES), :] = direction[:, at]
        sol_out[pl.ds(line, RHS, stride=LINES), :] = sol_new[:, at]
        res_out[pl.ds(line, RHS, stride=LINES), :] = res_new[:, at]


def build(mesh, xs):
    sizes = tuple(mesh.shape[a] for a in AXES)
    zs = sizes[0] // (CORES * xs) * sizes[2]
    slots = 1 + (xs * sizes[1] - 1) + len(window_offsets(zs)) + len(stride_offsets(zs))
    f32 = jnp.float32
    vmem = pl.BlockSpec(memory_space=pltpu.VMEM)

    def body(solution, residual, direction_prev, image_prev, gram_prev):
        flat = (RHS * LINES, LY)
        sol, res, dirp, imgp = (a.reshape(flat) for a in (solution, residual, direction_prev, image_prev))
        field = jax.ShapeDtypeStruct((LINES, RHS, LY), f32)
        dma = pltpu.SemaphoreType.DMA
        smooth, image, total, inverse = pl.pallas_call(
            functools.partial(exchange_kernel, sizes, xs),
            name="exchange",
            out_shape=(field, field, jax.ShapeDtypeStruct((8, 128), f32), jax.ShapeDtypeStruct((RHS, 128), f32)),
            in_specs=[vmem] * 4,
            out_specs=(vmem,) * 4,
            scratch_shapes=[
                pltpu.VMEM((3, N0, RHS, LY), f32),
                pltpu.VMEM((2, 3, N1, RHS, LY), f32),
                *[pltpu.VMEM((LZ, RHS, LY), f32)] * 4,
                pltpu.VMEM((N0, RHS, WIDE), f32),
                pltpu.VMEM((2, N1, RHS, WIDE), f32),
                pltpu.VMEM((LZ + 2, RHS, WIDE), f32),
                pltpu.VMEM((3, 2, RHS, WIDE), f32),
                pltpu.VMEM((LZ + 1, RHS, WIDE), f32),
                pltpu.VMEM((RHS, WIDE), f32),
                *[pltpu.VMEM((LZ, RHS, LY), f32)] * 2,
                pltpu.VMEM((4, 8, 128), f32),
                pltpu.VMEM((slots, 8, 128), f32),
                dma((8,)), dma((8,)), dma((2,)), dma((2,)), dma((2, 8)), dma((2, 8)), dma((2,)), dma((2,)),
                dma((slots,)), dma((slots,)),
            ],
            compiler_params=pltpu.CompilerParams(collective_id=0, has_side_effects=True),
        )(res, dirp, imgp, gram_prev)
        out = jax.ShapeDtypeStruct(flat, f32)
        sol_new, res_new, direction = pl.pallas_call(
            update_kernel,
            name="update",
            out_shape=(out, out, out),
            in_specs=[vmem] * 8,
            out_specs=(vmem,) * 3,
        )(sol, res, dirp, imgp, smooth, image, total, inverse)
        return tuple(a.reshape(solution.shape) for a in (sol_new, res_new, direction))

    field = P(None, "gx", "gz", "gy")
    return jax.shard_map(
        body, mesh=mesh, in_specs=(field,) * 4 + (P(),), out_specs=(field,) * 3, check_vma=False
    )


def solution(mesh):
    return build(mesh, xs=4)
```
